32 devices in a mesh: grp: 16 (over z, y, core), col: 2 (over x).
Axes of the slice: x: 2, y: 2, z: 4, core: 2. Of those that a mesh axis runs over, the one named last changes fastest.
Arguments:
- grad: float32 [4096, 16384], P('col', 'grp'), may hold values from -1.8 to 1.8
- exp_avg: float32 [4096, 16384], P('col', 'grp'), may hold values from -1.8 to 1.8
- exp_avg_sq: float32 [4096, 16384], P('col', 'grp'), may hold values from 0.01 to 0.36
- left_basis: bfloat16 [4096, 4096], P('grp', 'col'), may hold values from -1 to 1
- right_basis: bfloat16 [16384, 512], P('grp', 'col'), may hold values from -1 to 1
- gram_left: float32 [4096, 4096], P('grp', 'col'), may hold values from -6 to 6
- gram_right: float32 [16384, 512], P('grp', 'col'), may hold values from -6 to 6
Outputs:
- update: float32 [4096, 16384], P('col', 'grp')
- first_moment: float32 [4096, 16384], P('col', 'grp')
- second_moment: float32 [4096, 16384], P('col', 'grp')
- left_stat: float32 [4096, 4096], P('grp', 'col')
- right_stat: float32 [16384, 512], P('grp', 'col')
The draws below stay inside these ranges and needn't reach their ends.
All inputs are finite; a program needn't handle non-finite values.
Results may differ from the reference program's by a relative error of at most 0.0041.
Values may be sent and summed in bfloat16 or wider, within the bound.
No kernel may reach another device: no remote copies, remote signals or barrier semaphores. Data moves between devices by JAX's collectives and lax.ppermute only.
A program may use at most 256 MiB of HBM per device.

```python
import math
import jax
import jax.numpy as jnp
from jax import lax

M = 4096
N = 16384
RB = 512


def draw_left_basis(key, part):
    noise = jax.random.normal(jax.random.fold_in(key, 11), (M, M), jnp.float32)
    basis, upper = jnp.linalg.qr(noise)
    return basis.astype(jnp.bfloat16)


def draw_right_basis(key, part):
    noise = jax.random.normal(jax.random.fold_in(key, 23), (N // RB, RB, RB), jnp.float32)
    basis, upper = jnp.linalg.qr(noise)
    return basis.reshape(N, RB).astype(jnp.bfloat16)


def raised(entries, key, source, target, blocks, factor):
    owner, partner = [(jnp.arange(entries.shape[axis_at]) // (entries.shape[axis_at] // blocks)).reshape([-1 if axis == axis_at else 1 for axis in range(entries.ndim)]) for axis_at in (source, target)]
    chosen = jax.random.permutation(key, blocks)[partner]
    strong = (owner == chosen) | (owner == (partner + blocks // 2) % blocks)
    return jnp.where(strong, factor * entries, entries)


def block_scale(rng, shape, shards, least, largest):
    def one(dim, blocks):
        heights = jax.random.uniform(jax.random.fold_in(jax.random.fold_in(rng, 6), dim), (blocks,), jnp.float32, least / len(shards), largest / len(shards))
        return jnp.repeat(jnp.exp(heights), shape[dim] // blocks).reshape((-1,) + (1,) * (len(shape) - dim - 1))

    factor_of = one(*shards[0])
    for cut in shards[1:]:
        factor_of = factor_of * one(*cut)
    return factor_of


def gaussian(stream_key, extent, width, most, cuts=(), kind=jnp.bfloat16):
    entries = jax.random.normal(stream_key, extent, jnp.float32) * width
    if len(cuts) > 0:
        entries = block_scale(stream_key, extent, cuts, -0.22, 0.18) * entries
    return jnp.clip(entries, min=-most, max=most).astype(kind)


def gaussian_with(rng, extent, scale, bound, cuts, heavy, kind=jnp.bfloat16):
    drawn = scale * jax.random.normal(rng, extent, jnp.float32)
    if cuts:
        drawn = drawn * block_scale(rng, extent, cuts, -0.22, 0.18)
    return jnp.clip(raised(drawn, jax.random.fold_in(rng, 3), *heavy), -bound, bound).astype(kind)


def setup_inputs(seed: int = 0) -> dict:
    streams_of = jax.random.split(jax.random.key(seed), 8)
    grad = gaussian_with(streams_of[0], (M, N), 0.3, 1.8, ((0, 2), (1, 16)), (1, 0, 16, 2.0), jnp.float32)
    exp_avg = gaussian(streams_of[1], (M, N), 0.3, 1.8, ((0, 2), (1, 16)), jnp.float32)
    exp_avg_sq = jnp.clip(jnp.exp(math.log(0.36) - 3.583519 * jax.random.uniform(streams_of[2], (M, N), jnp.float32) ** block_scale(streams_of[2], (M, N), ((0, 2), (1, 16)), -0.2, 0.2)), 0.01, 0.36)
    left_basis = draw_left_basis(jax.random.fold_in(streams_of[7], 71), 0)
    right_basis = draw_right_basis(jax.random.fold_in(streams_of[7], 71), 0)
    gram_left = gaussian(streams_of[5], (M, M), 1.0, 6.0, ((0, 16), (1, 2)), jnp.float32)
    gram_right = gaussian(streams_of[6], (N, RB), 1.0, 6.0, ((0, 16), (1, 2)), jnp.float32)
    return dict(grad=grad, exp_avg=exp_avg, exp_avg_sq=exp_avg_sq, left_basis=left_basis, right_basis=right_basis, gram_left=gram_left, gram_right=gram_right)


decay = 0.95
bias_fix = 1.0 - decay ** 10

def reference(grad, exp_avg, exp_avg_sq, left_basis, right_basis, gram_left, gram_right):
    block_count = N // RB
    rounded = grad.astype(jnp.bfloat16)
    grad_blocks = rounded.reshape(M, block_count, RB).astype(jnp.float32)
    basis_blocks = right_basis.reshape(block_count, RB, RB).astype(jnp.float32)
    turned = jnp.einsum('mbj,bjr->mbr', grad_blocks, basis_blocks, precision=lax.Precision.HIGHEST)
    turned = turned.reshape(M, N).astype(jnp.bfloat16)
    rotated = jnp.dot(left_basis.T.astype(jnp.float32), turned.astype(jnp.float32), preferred_element_type=jnp.float32)
    first_moment = decay * exp_avg + (1.0 - decay) * rotated
    second_moment = decay * exp_avg_sq + (1.0 - decay) * rotated * rotated
    direction = (first_moment / bias_fix / (jnp.sqrt(second_moment / bias_fix) + 1e-08)).astype(jnp.bfloat16)
    back = jnp.dot(left_basis.astype(jnp.float32), direction.astype(jnp.float32), preferred_element_type=jnp.float32).astype(jnp.bfloat16)
    back_blocks = back.reshape(M, block_count, RB).astype(jnp.float32)
    update = jnp.einsum('mbr,bjr->mbj', back_blocks, basis_blocks, precision=lax.Precision.HIGHEST).reshape(M, N)
    left_stat = decay * gram_left + (1.0 - decay) * jnp.dot(rounded.astype(jnp.float32), rounded.T.astype(jnp.float32), preferred_element_type=jnp.float32)
    right_term = jnp.einsum('mbj,mbr->bjr', grad_blocks, grad_blocks, precision=lax.Precision.HIGHEST).reshape(N, RB)
    right_stat = decay * gram_right + (1.0 - decay) * right_term
    return (update, first_moment, second_moment, left_stat, right_stat)
```

```python
import functools

import jax
import jax.numpy as jnp
from jax import lax
from jax.experimental import pallas as pl
from jax.experimental.pallas import tpu as pltpu
from jax.sharding import PartitionSpec as P


RB = 512

decay = 0.95
bias_fix = 1.0 - decay**10

F32 = jnp.float32
BF16 = jnp.bfloat16
ANY = pl.BlockSpec(memory_space=pl.ANY)


def params(grid_rank=1):
    return pltpu.CompilerParams(
        dimension_semantics=("arbitrary",) * grid_rank, vmem_limit_bytes=58 * 2**20
    )


def cost(flops, moved):
    return pl.CostEstimate(flops=flops, bytes_accessed=moved, transcendentals=0)


def dot(a, b, ca, cb):
    return lax.dot_general(a, b, (((ca,), (cb,)), ((), ())), preferred_element_type=F32)


def scalars(*values):
    return jnp.stack([jnp.asarray(v, jnp.int32) for v in values])


def blank(shape, kind):
    return pl.pallas_call(
        lambda out: None, out_shape=jax.ShapeDtypeStruct(shape, kind), out_specs=ANY, name="blank"
    )()


def block_kernel(pieces, sections, fill, turn, strips, s_ref, at_ref, *refs):
    lefts, refs = refs[:pieces], refs[pieces:]
    right, refs = refs[0], refs[1:]
    grads, refs = refs[:sections], refs[sections:]
    avg, avg_sq = refs[:2]
    first_out, second_out, other_out, own_out, left, turned, direction, sems = refs[-8:]
    part, tile = grads[0].shape[0], avg.shape[0]
    strip = own_out.shape[0]
    step = pl.program_id(0)
    lead = sections * fill

    def load(c):
        lanes = pl.ds(c * tile, tile)
        for k in range(pieces):
            rows = lefts[k].shape[0]
            base = pl.multiple_of(at_ref[k], 16)
            pltpu.make_async_copy(lefts[k].at[:, lanes], left.at[pl.ds(base, rows), lanes], sems.at[c]).start()

    for c in range(turn):

        @pl.when(step == min(c, lead - 1))
        def _(c=c):
            load(c)

    for k in range(sections):

        @pl.when((step >= k * fill) & (step < (k + 1) * fill))
        def _(k=k):
            base = pl.multiple_of((s_ref[k] * fill + step - k * fill) * part, part)
            turned[pl.ds(base, part), :] = dot(grads[k][...], right[...], 1, 0).astype(BF16)

    for c in range(turn):

        @pl.when(step == lead + c)
        def _(c=c):
            lanes = pl.ds(c * tile, tile)
            pltpu.make_async_copy(left.at[:, lanes], left.at[:, lanes], sems.at[c]).wait()
            rotated = dot(left[:, lanes], turned[...], 0, 0)
            first = decay * avg[...] + (1.0 - decay) * rotated
            second = decay * avg_sq[...] + (1.0 - decay) * rotated * rotated
            first_out[...] = first
            second_out[...] = second
            direction[lanes, :] = (
                first / bias_fix / (jnp.sqrt(second / bias_fix) + 1e-08)
            ).astype(BF16)

    spin = step - lead - turn
    split = (sections - 1) * strips

    @pl.when(spin >= 0)
    def _():
        section = s_ref[lax.rem(spin // strips + 1, sections)]
        base = pl.multiple_of((section * strips + lax.rem(spin, strips)) * strip, strip)
        share = dot(left[pl.ds(base, strip), :], direction[...], 1, 0)

        @pl.when(spin < split)
        def _():
            other_out[...] = share.astype(BF16)

        @pl.when(spin >= split)
        def _():
            own_out[...] = share


def block(b, order, left, right, grads, avg, avg_sq, old, after=()):
    places, lefts = left
    pieces = len(lefts)
    width = lefts[0].shape[1]
    rows, cols = avg.shape
    sections = len(grads)
    height = sections * rows
    part, tile, strip = min(512, rows), min(512, rows), min(512, rows)
    fill, turn, strips = rows // part, rows // tile, rows // strip
    lead = sections * fill
    split = max(sections - 1, 1) * strips

    def column(i, s, a):
        return (jnp.clip(i - lead, 0, turn - 1), b)

    def part_of(k):
        return lambda i, s, a: (jnp.clip(i - k * fill, 0, fill - 1), 0)

    in_specs = [
        *[ANY] * pieces,
        pl.BlockSpec((RB, RB), lambda i, s, a: (b, 0)),
        *[pl.BlockSpec((part, RB), part_of(k)) for k in range(sections)],
        pl.BlockSpec((tile, RB), column),
        pl.BlockSpec((tile, RB), column),
    ]
    args = [order, places, *lefts, right, *grads, avg, avg_sq]
    aliases = {}
    if old is not None:
        in_specs += [ANY, ANY]
        aliases = {len(args): 0, len(args) + 1: 1}
        args += list(old)
    in_specs += [ANY] * len(after)
    args += list(after)
    return pl.pallas_call(
        functools.partial(block_kernel, pieces, sections, fill, turn, strips),
        grid_spec=pltpu.PrefetchScalarGridSpec(
            num_scalar_prefetch=2,
            grid=(lead + turn + sections * strips,),
            in_specs=in_specs,
            out_specs=[
                pl.BlockSpec((tile, RB), column),
                pl.BlockSpec((tile, RB), column),
                pl.BlockSpec((strip, RB), lambda i, s, a: (jnp.clip(i - lead - turn, 0, split - 1), 0)),
                pl.BlockSpec(
                    (strip, RB), lambda i, s, a: (jnp.clip(i - lead - turn - split, 0, strips - 1), 0)
                ),
            ],
            scratch_shapes=[
                pltpu.VMEM((height, width), BF16),
                pltpu.VMEM((height, RB), BF16),
                pltpu.VMEM((rows, RB), BF16),
                pltpu.SemaphoreType.DMA((turn,)),
            ],
        ),
        out_shape=[
            jax.ShapeDtypeStruct((rows, cols), F32),
            jax.ShapeDtypeStruct((rows, cols), F32),
            jax.ShapeDtypeStruct((split * strip, RB), BF16),
            jax.ShapeDtypeStruct((rows, RB), F32),
        ],
        input_output_aliases=aliases,
        compiler_params=params(),
        cost_estimate=cost(4 * height * RB * (rows + RB), 2 * height * (width + RB) + 24 * rows * RB),
        name="block",
    )(*args)


def update_kernel(count, own, right, *refs):
    total = own[...]
    for part in refs[:count]:
        total = total + part[...].astype(F32)
    refs[-1][...] = dot(total.astype(BF16), right[...], 1, 1)


def update_block(b, own, parts, right, cols, old, after=()):
    rows = own.shape[0]
    tile = min(512, rows)
    row = lambda i: (i, 0)
    in_specs = [
        pl.BlockSpec((tile, RB), row),
        pl.BlockSpec((RB, RB), lambda i: (b, 0)),
        *[pl.BlockSpec((tile, RB), row)] * len(parts),
    ]
    args = [own, right, *parts]
    aliases = {}
    if old is not None:
        in_specs.append(ANY)
        aliases = {len(args): 0}
        args.append(old)
    in_specs += [ANY] * len(after)
    args += list(after)
    return pl.pallas_call(
        functools.partial(update_kernel, len(parts)),
        grid=(rows // tile,),
        in_specs=in_specs,
        out_specs=pl.BlockSpec((tile, RB), lambda i: (i, b)),
        out_shape=jax.ShapeDtypeStruct((rows, cols), F32),
        input_output_aliases=aliases,
        compiler_params=params(),
        cost_estimate=cost(2 * rows * RB * RB, rows * RB * 10),
        name="update",
    )(*args)


def gram_kernel(pieces, s_ref, *refs):
    total = None
    for k in range(pieces):
        term = dot(refs[k][...], refs[pieces + k][...], 1, 1)
        total = term if total is None else total + term
    refs[-1][0] = total.astype(BF16)


def left_gram(section, core, slab, count, tops, sides, old, after=()):
    rows, width = tops[0].shape
    pieces = len(tops)
    steps = rows // (2 * slab)
    in_specs = [
        *[pl.BlockSpec((slab, width), lambda i, s: (2 * i + s[1], 0))] * pieces,
        *[pl.BlockSpec((rows, width), lambda i, s: (0, 0))] * pieces,
    ]
    args = [scalars(section, core), *tops, *sides]
    aliases = {}
    if old is not None:
        in_specs.append(ANY)
        aliases = {len(args): 0}
        args.append(old)
    in_specs += [ANY] * len(after)
    args += list(after)
    return pl.pallas_call(
        functools.partial(gram_kernel, pieces),
        grid_spec=pltpu.PrefetchScalarGridSpec(
            num_scalar_prefetch=1,
            grid=(steps,),
            in_specs=in_specs,
            out_specs=pl.BlockSpec((1, slab, rows), lambda i, s: (s[0] * steps + i, 0, 0)),
        ),
        out_shape=jax.ShapeDtypeStruct((count, slab, rows), BF16),
        input_output_aliases=aliases,
        compiler_params=params(),
        cost_estimate=cost(rows * rows * width * pieces, rows * width * 3 * pieces + 2 * rows * rows),
        name="left_gram",
    )(*args)


def right_kernel(sections, s_ref, gram, *refs):
    out, total = refs[-2:]
    step = pl.program_id(0)

    @pl.when(step == 0)
    def _():
        total[...] = jnp.zeros_like(total)

    for k in range(sections):
        total[...] += dot(refs[2 * k][...], refs[2 * k + 1][...], 0, 0)

    @pl.when(step == pl.num_programs(0) - 1)
    def _():
        out[...] = decay * gram[...] + (1.0 - decay) * total[...]


def right_stat_block(b, place, gram, grads, old, after=()):
    rows = grads[0].shape[0]
    share = gram.shape[1]
    tile = min(512, rows)
    in_specs = [pl.BlockSpec((RB, share), lambda i, s: (b, 0))]
    args = [scalars(place), gram]
    lanes = share % 128 == 0
    for g in grads:
        in_specs += [
            pl.BlockSpec((tile, RB), lambda i, s: (i, 0)),
            pl.BlockSpec((tile, share), (lambda i, s: (i, s[0])) if lanes else (lambda i, s: (i, 0))),
        ]
        args += [g, g if lanes else lax.dynamic_slice_in_dim(g, place * share, share, 1)]
    aliases = {}
    if old is not None:
        in_specs.append(ANY)
        aliases = {len(args): 0}
        args.append(old)
    in_specs += [ANY] * len(after)
    args += list(after)
    return pl.pallas_call(
        functools.partial(right_kernel, len(grads)),
        grid_spec=pltpu.PrefetchScalarGridSpec(
            num_scalar_prefetch=1,
            grid=(rows // tile,),
            in_specs=in_specs,
            out_specs=pl.BlockSpec((RB, share), lambda i, s: (b, 0)),
            scratch_shapes=[pltpu.VMEM((RB, share), F32)],
        ),
        out_shape=jax.ShapeDtypeStruct(gram.shape, F32),
        input_output_aliases=aliases,
        compiler_params=params(),
        cost_estimate=cost(2 * rows * len(grads) * RB * share, rows * len(grads) * RB * 4),
        name="right_stat",
    )(*args)


class Places:
    def __init__(self):
        self.count = lax.axis_size("grp")
        self.outer = self.count // 4
        index = lax.axis_index("grp")
        self.z, self.y, self.core = index // 4, (index // 2) % 2, index % 2

    def send(self, x, dz=0, dy=0, dcore=0):
        pairs = []
        for i in range(self.count):
            z, y, core = i // 4, (i // 2) % 2, i % 2
            pairs.append((i, ((z + dz) % self.outer) * 4 + (y ^ dy) * 2 + (core ^ dcore)))
        return lax.ppermute(x, "grp", pairs)

    def pass_on(self, x, dz=0, dy=0, only=0):
        pairs = []
        for i in range(self.count):
            z, y, core = i // 4, (i // 2) % 2, i % 2
            if 0 <= z + only < self.outer:
                pairs.append((i, (z + dz) * 4 + (y ^ dy) * 2 + core))
        return lax.ppermute(x, "grp", pairs)

    def chip(self, dz, dy):
        return ((self.z + dz) % self.outer) * 2 + (self.y ^ dy)


def thirds(rows):
    a = rows // 16 // 3 * 16
    a = max(a, 16)
    return [(0, rows - 2 * a), (rows - 2 * a, a), (rows - a, a)]


def gather_left(at, left_basis):
    slab = left_basis.shape[0]
    far = at.outer // 2
    rows, pieces = [], []

    def send(x, **how):
        return at.send(x, **how)

    def put(x, dz, dy, start=0):
        for piece, core in ((x, at.core), (send(x, dcore=1), 1 - at.core)):
            rows.append((at.chip(dz, dy) * 2 + core) * slab + start)
            pieces.append(piece)

    got = {(0, 0): left_basis}
    got[0, 1] = send(left_basis, dy=1)
    for d in range(1, far + 1):
        got[d, 0] = send(got[d - 1, 0], dz=-1)
        if d < far:
            got[-d, 0] = send(got[1 - d, 0], dz=1)
            got[-d, 1] = send(got[1 - d, 1], dz=1)
            got[d, 1] = send(got[d, 0], dy=1)
    for key, x in got.items():
        put(x, *key)
    cut = thirds(slab)
    sources = ((got[far, 0], dict(dy=1)), (got[1 - far, 1], dict(dz=1)), (got[far - 1, 1], dict(dz=-1)))
    for (start, size), (source, how) in zip(cut, sources, strict=True):
        put(send(source[start : start + size], **how), far, 1, start)
    return scalars(*rows), pieces


class Reduction:
    def __init__(self, at, parts):
        self.at, self.parts = at, parts
        self.offsets = [dz for t in range(at.outer - 1, 0, -1) for dz in (t, -t)] + [0]
        self.came = {}
        for dz in self.offsets:
            self.came[dz] = [at.pass_on(self.part(dz, 1), dy=1, only=dz)]

    def part(self, dz, dy):
        return lax.dynamic_index_in_dim(self.parts, self.at.chip(dz, dy), 0, keepdims=False)

    def total(self, dz):
        total = self.part(dz, 0).astype(F32)
        for x in self.came[dz]:
            total = total + x.astype(F32)
        return total

    def round(self, t, after):
        self.parts, _ = lax.optimization_barrier((self.parts, after))
        sent = []
        for dz, way in ((t, 1), (-t, -1)):
            sent.append(self.total(dz).astype(BF16))
            self.came[dz - way].append(self.at.pass_on(sent[-1], dz=way, only=dz))
        return tuple(sent)


def step(grad, exp_avg, exp_avg_sq, left_basis, right_basis, gram_left, gram_right):
    at = Places()
    col_count = lax.axis_size("col")
    mine = lax.axis_index("col")
    rows_here, cols_here = grad.shape
    blocks = range(cols_here // RB)
    others = range(1, col_count)
    slab = gram_left.shape[0]

    def from_right(x, s):
        return lax.ppermute(x, "col", [((i + s) % col_count, i) for i in range(col_count)])

    def to_right(x, s):
        return lax.ppermute(x, "col", [(i, (i + s) % col_count) for i in range(col_count)])

    def twin(x):
        return at.send(x, dcore=1)

    shares = [right_basis] + [from_right(right_basis, s) for s in others]
    own = [grad[:, b * RB : (b + 1) * RB].astype(BF16) for b in blocks]
    grads = [[own[b]] + [from_right(own[b], s) for s in others] for b in blocks]
    sections = [(mine + s) % col_count for s in range(col_count)]
    share = right_basis.shape[1]
    right = blank((cols_here, RB), BF16)
    for s in range(col_count):
        right = lax.dynamic_update_slice(right, shares[s], (0, sections[s] * share))
    order = scalars(*sections)

    left = gather_left(at, left_basis)

    twins = [[twin(x) for x in grads[b]] for b in blocks]
    sides = [grads[b][0] for b in blocks] + [twins[b][0] for b in blocks]
    parts = moments = update = right_stat = None
    kept, came, after = [], [], ()
    for s in range(col_count):
        tops = [grads[k][s] for k in blocks] + [twins[k][s] for k in blocks]
        parts = left_gram(sections[s], at.core, slab, at.count // 2, tops, sides, parts)
    sums = Reduction(at, parts)
    rounds = list(range(at.outer - 1, 0, -1))
    after = (parts,)
    for b in blocks:
        first, second, shared, share = block(
            b, order, left, right, grads[b], exp_avg, exp_avg_sq, moments, after
        )
        moments = (first, second)
        kept.append(share)
        came.append([to_right(shared[(s - 1) * rows_here : s * rows_here], s) for s in others])
        after = sums.round(rounds.pop(0), share) if rounds else (share,)
    for b in blocks:
        right_stat = right_stat_block(b, mine, gram_right, grads[b], right_stat, after)
    for b in blocks[:-1]:
        update = update_block(b, kept[b], came[b], right, cols_here, update, after)
    while rounds:
        after = sums.round(rounds.pop(0), right_stat)
    left_stat = decay * gram_left + (1.0 - decay) * sums.total(0)
    update = update_block(blocks[-1], kept[-1], came[-1], right, cols_here, update, after)
    return (update, *moments, left_stat, right_stat)


def solution(mesh):
    return jax.shard_map(
        step,
        mesh=mesh,
        in_specs=(
            P("col", "grp"),
            P("col", "grp"),
            P("col", "grp"),
            P("grp", "col"),
            P("grp", "col"),
            P("grp", "col"),
            P("grp", "col"),
        ),
        out_specs=(
            P("col", "grp"),
            P("col", "grp"),
            P("col", "grp"),
            P("grp", "col"),
            P("grp", "col"),
        ),
        check_vma=False,
    )
```

```python
import functools

import jax
import jax.numpy as jnp
from jax import lax
from jax.experimental import pallas as pl
from jax.experimental.pallas import tpu as pltpu
from jax.sharding import PartitionSpec as P


RB = 512

decay = 0.95
bias_fix = 1.0 - decay**10

F32 = jnp.float32
BF16 = jnp.bfloat16
ANY = pl.BlockSpec(memory_space=pl.ANY)


def params(grid_rank=1):
    return pltpu.CompilerParams(
        dimension_semantics=("arbitrary",) * grid_rank, vmem_limit_bytes=58 * 2**20
    )


def cost(flops, moved):
    return pl.CostEstimate(flops=flops, bytes_accessed=moved, transcendentals=0)


def dot(a, b, ca, cb):
    return lax.dot_general(a, b, (((ca,), (cb,)), ((), ())), preferred_element_type=F32)


def scalars(*values):
    return jnp.stack([jnp.asarray(v, jnp.int32) for v in values])


def blank(shape, kind):
    return pl.pallas_call(
        lambda out: None, out_shape=jax.ShapeDtypeStruct(shape, kind), out_specs=ANY, name="blank"
    )()


def block_kernel(pieces, sections, fill, turn, strips, s_ref, at_ref, *refs):
    lefts, refs = refs[:pieces], refs[pieces:]
    right, refs = refs[0], refs[1:]
    grads, refs = refs[:sections], refs[sections:]
    avg, avg_sq = refs[:2]
    first_out, second_out, other_out, own_out, left, turned, direction, sems = refs[-8:]
    part, tile = grads[0].shape[0], avg.shape[0]
    strip = own_out.shape[0]
    step = pl.program_id(0)
    lead = sections * fill

    @pl.when((step == 0) | ((step >= lead - 1) & (step < lead + turn - 2)))
    def _():
        c = jnp.where(step == 0, 0, step - lead + 2)
        lanes = pl.ds(pl.multiple_of(c * tile, tile), tile)
        for k in range(pieces):
            rows = lefts[k].shape[0]
            base = pl.multiple_of(at_ref[k], 16)
            pltpu.make_async_copy(
                lefts[k].at[:, lanes], left.at[pl.ds(base, rows), lanes], sems.at[c]
            ).start()

    for k in range(sections):

        @pl.when((step >= k * fill) & (step < (k + 1) * fill))
        def _(k=k):
            base = pl.multiple_of((s_ref[k] * fill + step - k * fill) * part, part)
            turned[pl.ds(base, part), :] = dot(grads[k][...], right[...], 1, 0).astype(BF16)

    @pl.when((step >= lead) & (step < lead + turn))
    def _():
        c = step - lead
        lanes = pl.ds(pl.multiple_of(c * tile, tile), tile)
        pltpu.make_async_copy(left.at[:, lanes], left.at[:, lanes], sems.at[c]).wait()
        rotated = dot(left[:, lanes], turned[...], 0, 0)
        first = decay * avg[...] + (1.0 - decay) * rotated
        second = decay * avg_sq[...] + (1.0 - decay) * rotated * rotated
        first_out[...] = first
        second_out[...] = second
        direction[lanes, :] = (
            first * (1.0 / bias_fix) / (jnp.sqrt(second * (1.0 / bias_fix)) + 1e-08)
        ).astype(BF16)

    spin = step - lead - turn
    split = (sections - 1) * strips

    @pl.when(spin >= 0)
    def _():
        section = s_ref[lax.rem(spin // strips + 1, sections)]
        base = pl.multiple_of((section * strips + lax.rem(spin, strips)) * strip, strip)
        share = dot(left[pl.ds(base, strip), :], direction[...], 1, 0)

        @pl.when(spin < split)
        def _():
            other_out[...] = share.astype(BF16)

        @pl.when(spin >= split)
        def _():
            own_out[...] = share


def block(b, order, left, right, grads, avg, avg_sq, old, after=()):
    places, lefts = left
    pieces = len(lefts)
    width = lefts[0].shape[1]
    rows, cols = avg.shape
    sections = len(grads)
    height = sections * rows
    part, tile, strip = min(512, rows), min(512, rows), min(512, rows)
    fill, turn, strips = rows // part, rows // tile, rows // strip
    lead = sections * fill
    split = max(sections - 1, 1) * strips
    assert lead > 1

    def column(i, s, a):
        return (jnp.clip(i - lead, 0, turn - 1), b)

    def part_of(k):
        return lambda i, s, a: (jnp.clip(i - k * fill, 0, fill - 1), 0)

    in_specs = [
        *[ANY] * pieces,
        pl.BlockSpec((RB, RB), lambda i, s, a: (b, 0)),
        *[pl.BlockSpec((part, RB), part_of(k)) for k in range(sections)],
        pl.BlockSpec((tile, RB), column),
        pl.BlockSpec((tile, RB), column),
    ]
    args = [order, places, *lefts, right, *grads, avg, avg_sq]
    aliases = {}
    if old is not None:
        in_specs += [ANY, ANY]
        aliases = {len(args): 0, len(args) + 1: 1}
        args += list(old)
    in_specs += [ANY] * len(after)
    args += list(after)
    return pl.pallas_call(
        functools.partial(block_kernel, pieces, sections, fill, turn, strips),
        grid_spec=pltpu.PrefetchScalarGridSpec(
            num_scalar_prefetch=2,
            grid=(lead + turn + sections * strips,),
            in_specs=in_specs,
            out_specs=[
                pl.BlockSpec((tile, RB), column),
                pl.BlockSpec((tile, RB), column),
                pl.BlockSpec((strip, RB), lambda i, s, a: (jnp.clip(i - lead - turn, 0, split - 1), 0)),
                pl.BlockSpec(
                    (strip, RB), lambda i, s, a: (jnp.clip(i - lead - turn - split, 0, strips - 1), 0)
                ),
            ],
            scratch_shapes=[
                pltpu.VMEM((height, width), BF16),
                pltpu.VMEM((height, RB), BF16),
                pltpu.VMEM((rows, RB), BF16),
                pltpu.SemaphoreType.DMA((turn,)),
            ],
        ),
        out_shape=[
            jax.ShapeDtypeStruct((rows, cols), F32),
            jax.ShapeDtypeStruct((rows, cols), F32),
            jax.ShapeDtypeStruct((split * strip, RB), BF16),
            jax.ShapeDtypeStruct((rows, RB), F32),
        ],
        input_output_aliases=aliases,
        compiler_params=params(),
        cost_estimate=cost(4 * height * RB * (rows + RB), 2 * height * (width + RB) + 24 * rows * RB),
        name="block",
    )(*args)


def update_kernel(count, own, right, *refs):
    total = own[...]
    for part in refs[:count]:
        total = total + part[...].astype(F32)
    refs[-1][...] = dot(total.astype(BF16), right[...], 1, 1)


def update_block(b, own, parts, right, cols, old, after=()):
    rows = own.shape[0]
    tile = min(512, rows)
    row = lambda i: (i, 0)
    in_specs = [
        pl.BlockSpec((tile, RB), row),
        pl.BlockSpec((RB, RB), lambda i: (b, 0)),
        *[pl.BlockSpec((tile, RB), row)] * len(parts),
    ]
    args = [own, right, *parts]
    aliases = {}
    if old is not None:
        in_specs.append(ANY)
        aliases = {len(args): 0}
        args.append(old)
    in_specs += [ANY] * len(after)
    args += list(after)
    return pl.pallas_call(
        functools.partial(update_kernel, len(parts)),
        grid=(rows // tile,),
        in_specs=in_specs,
        out_specs=pl.BlockSpec((tile, RB), lambda i: (i, b)),
        out_shape=jax.ShapeDtypeStruct((rows, cols), F32),
        input_output_aliases=aliases,
        compiler_params=params(),
        cost_estimate=cost(2 * rows * RB * RB, rows * RB * 10),
        name="update",
    )(*args)


def gram_kernel(pieces, s_ref, *refs):
    total = None
    for k in range(pieces):
        term = dot(refs[k][...], refs[pieces + k][...], 1, 1)
        total = term if total is None else total + term
    refs[-1][0] = total.astype(BF16)


def left_gram(section, core, slab, count, tops, sides, old, after=()):
    rows, width = tops[0].shape
    pieces = len(tops)
    steps = rows // (2 * slab)
    in_specs = [
        *[pl.BlockSpec((slab, width), lambda i, s: (2 * i + s[1], 0))] * pieces,
        *[pl.BlockSpec((rows, width), lambda i, s: (0, 0))] * pieces,
    ]
    args = [scalars(section, core), *tops, *sides]
    aliases = {}
    if old is not None:
        in_specs.append(ANY)
        aliases = {len(args): 0}
        args.append(old)
    in_specs += [ANY] * len(after)
    args += list(after)
    return pl.pallas_call(
        functools.partial(gram_kernel, pieces),
        grid_spec=pltpu.PrefetchScalarGridSpec(
            num_scalar_prefetch=1,
            grid=(steps,),
            in_specs=in_specs,
            out_specs=pl.BlockSpec((1, slab, rows), lambda i, s: (s[0] * steps + i, 0, 0)),
        ),
        out_shape=jax.ShapeDtypeStruct((count, slab, rows), BF16),
        input_output_aliases=aliases,
        compiler_params=params(),
        cost_estimate=cost(rows * rows * width * pieces, rows * width * 3 * pieces + 2 * rows * rows),
        name="left_gram",
    )(*args)


def right_kernel(sections, s_ref, gram, *refs):
    out, total = refs[-2:]
    step = pl.program_id(0)

    @pl.when(step == 0)
    def _():
        total[...] = jnp.zeros_like(total)

    for k in range(sections):
        total[...] += dot(refs[2 * k][...], refs[2 * k + 1][...], 0, 0)

    @pl.when(step == pl.num_programs(0) - 1)
    def _():
        out[...] = decay * gram[...] + (1.0 - decay) * total[...]


def right_stat_block(b, place, gram, grads, old, after=()):
    rows = grads[0].shape[0]
    share = gram.shape[1]
    tile = min(512, rows)
    in_specs = [pl.BlockSpec((RB, share), lambda i, s: (b, 0))]
    args = [scalars(place), gram]
    lanes = share % 128 == 0
    for g in grads:
        in_specs += [
            pl.BlockSpec((tile, RB), lambda i, s: (i, 0)),
            pl.BlockSpec((tile, share), (lambda i, s: (i, s[0])) if lanes else (lambda i, s: (i, 0))),
        ]
        args += [g, g if lanes else lax.dynamic_slice_in_dim(g, place * share, share, 1)]
    aliases = {}
    if old is not None:
        in_specs.append(ANY)
        aliases = {len(args): 0}
        args.append(old)
    in_specs += [ANY] * len(after)
    args += list(after)
    return pl.pallas_call(
        functools.partial(right_kernel, len(grads)),
        grid_spec=pltpu.PrefetchScalarGridSpec(
            num_scalar_prefetch=1,
            grid=(rows // tile,),
            in_specs=in_specs,
            out_specs=pl.BlockSpec((RB, share), lambda i, s: (b, 0)),
            scratch_shapes=[pltpu.VMEM((RB, share), F32)],
        ),
        out_shape=jax.ShapeDtypeStruct(gram.shape, F32),
        input_output_aliases=aliases,
        compiler_params=params(),
        cost_estimate=cost(2 * rows * len(grads) * RB * share, rows * len(grads) * RB * 4),
        name="right_stat",
    )(*args)


class Places:
    def __init__(self):
        self.count = lax.axis_size("grp")
        self.outer = self.count // 4
        index = lax.axis_index("grp")
        self.z, self.y, self.core = index // 4, (index // 2) % 2, index % 2

    def send(self, x, dz=0, dy=0, dcore=0):
        pairs = []
        for i in range(self.count):
            z, y, core = i // 4, (i // 2) % 2, i % 2
            pairs.append((i, ((z + dz) % self.outer) * 4 + (y ^ dy) * 2 + (core ^ dcore)))
        return lax.ppermute(x, "grp", pairs)

    def pass_on(self, x, dz=0, dy=0, only=0):
        pairs = []
        for i in range(self.count):
            z, y, core = i // 4, (i // 2) % 2, i % 2
            if 0 <= z + only < self.outer:
                pairs.append((i, (z + dz) * 4 + (y ^ dy) * 2 + core))
        return lax.ppermute(x, "grp", pairs)

    def chip(self, dz, dy):
        return ((self.z + dz) % self.outer) * 2 + (self.y ^ dy)


def thirds(rows):
    a = rows // 16 // 3 * 16
    a = max(a, 16)
    return [(0, rows - 2 * a), (rows - 2 * a, a), (rows - a, a)]


def gather_left(at, left_basis):
    slab = left_basis.shape[0]
    far = at.outer // 2
    rows, pieces = [], []

    def send(x, **how):
        return at.send(x, **how)

    def put(x, dz, dy, start=0):
        for piece, core in ((x, at.core), (send(x, dcore=1), 1 - at.core)):
            rows.append((at.chip(dz, dy) * 2 + core) * slab + start)
            pieces.append(piece)

    got = {(0, 0): left_basis}
    got[0, 1] = send(left_basis, dy=1)
    for d in range(1, far + 1):
        got[d, 0] = send(got[d - 1, 0], dz=-1)
        if d < far:
            got[-d, 0] = send(got[1 - d, 0], dz=1)
            got[-d, 1] = send(got[1 - d, 1], dz=1)
            got[d, 1] = send(got[d, 0], dy=1)
    for key, x in got.items():
        put(x, *key)
    cut = thirds(slab)
    sources = ((got[far, 0], dict(dy=1)), (got[1 - far, 1], dict(dz=1)), (got[far - 1, 1], dict(dz=-1)))
    for (start, size), (source, how) in zip(cut, sources, strict=True):
        put(send(source[start : start + size], **how), far, 1, start)
    return scalars(*rows), pieces


class Reduction:
    def __init__(self, at, sections):
        self.at, self.sections = at, sections
        self.came = {dz: [] for dz in range(1 - at.outer, at.outer)}
        self.across = []

    def add(self, s, parts):
        at, section, mine = self.at, self.sections[s], self.sections[0]
        self.parts = parts
        count = at.outer // len(self.sections)
        sent = []
        for k in range(count):
            step = jnp.where(section > mine, count - 1 - k, k)
            place = section * count + step
            slab = lax.dynamic_index_in_dim(parts, place * 2 + 1 - at.y, 0, keepdims=False)
            self.across.append((s, k, place, at.send(slab, dy=1)))
            sent.append(slab)
        return tuple(sent)

    def held(self, dz):
        outer = self.at.outer
        place = jnp.clip(self.at.z + dz, 0, outer - 1)
        total = lax.dynamic_index_in_dim(self.parts, place * 2 + self.at.y, 0, keepdims=False).astype(F32)
        across = None
        for s, k, where, x in self.across:
            if s > 0 and k > 0 and abs(dz) == outer - 1:
                continue
            across = x if across is None else jnp.where(place == where, x, across)
        return total + across.astype(F32)

    def arrived(self, total, dz, scale=1.0):
        for x in self.came[dz]:
            total = total + scale * x.astype(F32)
        return total

    def round(self, t, after):
        self.parts, _ = lax.optimization_barrier((self.parts, after))
        sent = []
        for dz, way in ((t, 1), (-t, -1)):
            total = self.held(dz)
            if t == 1:
                total = lax.optimization_barrier(total)
            sent.append(self.arrived(total, dz).astype(BF16))
            self.came[dz - way].append(self.at.pass_on(sent[-1], dz=way, only=dz))
        return tuple(sent)


def step(grad, exp_avg, exp_avg_sq, left_basis, right_basis, gram_left, gram_right):
    at = Places()
    col_count = lax.axis_size("col")
    mine = lax.axis_index("col")
    rows_here, cols_here = grad.shape
    blocks = range(cols_here // RB)
    others = range(1, col_count)
    slab = gram_left.shape[0]

    def from_right(x, s):
        return lax.ppermute(x, "col", [((i + s) % col_count, i) for i in range(col_count)])

    def to_right(x, s):
        return lax.ppermute(x, "col", [(i, (i + s) % col_count) for i in range(col_count)])

    def twin(x):
        return at.send(x, dcore=1)

    shares = [right_basis] + [from_right(right_basis, s) for s in others]
    own = [grad[:, b * RB : (b + 1) * RB].astype(BF16) for b in blocks]
    grads = [[own[b]] + [from_right(own[b], s) for s in others] for b in blocks]
    sections = [(mine + s) % col_count for s in range(col_count)]
    share = right_basis.shape[1]
    right = blank((cols_here, RB), BF16)
    for s in range(col_count):
        right = lax.dynamic_update_slice(right, shares[s], (0, sections[s] * share))
    order = scalars(*sections)

    left = gather_left(at, left_basis)

    twins = [[twin(x) for x in grads[b]] for b in blocks]
    sides = [grads[b][0] for b in blocks] + [twins[b][0] for b in blocks]
    parts = moments = update = right_stat = None
    kept, came, after = [], [], ()
    sums = Reduction(at, sections)
    for s in range(col_count):
        tops = [grads[k][s] for k in blocks] + [twins[k][s] for k in blocks]
        parts = left_gram(sections[s], at.core, slab, at.count // 2, tops, sides, parts, after)
        after = sums.add(s, parts)
    rounds = list(range(at.outer - 1, 0, -1))
    for b in blocks:
        first, second, shared, share = block(
            b, order, left, right, grads[b], exp_avg, exp_avg_sq, moments, after
        )
        moments = (first, second)
        kept.append(share)
        came.append([to_right(shared[(s - 1) * rows_here : s * rows_here], s) for s in others])
        after = sums.round(rounds.pop(0), share) if rounds else (share,)
    for b in blocks:
        right_stat = right_stat_block(b, mine, gram_right, grads[b], right_stat, after)
    for b in blocks[:-1]:
        update = update_block(b, kept[b], came[b], right, cols_here, update, after)
    while rounds:
        after = sums.round(rounds.pop(0), right_stat)
    base = lax.optimization_barrier(decay * gram_left + (1.0 - decay) * sums.held(0))
    left_stat = sums.arrived(base, 0, 1.0 - decay)
    update = update_block(blocks[-1], kept[-1], came[-1], right, cols_here, update, after)
    return (update, *moments, left_stat, right_stat)


def solution(mesh):
    return jax.shard_map(
        step,
        mesh=mesh,
        in_specs=(
            P("col", "grp"),
            P("col", "grp"),
            P("col", "grp"),
            P("grp", "col"),
            P("grp", "col"),
            P("grp", "col"),
            P("grp", "col"),
        ),
        out_specs=(
            P("col", "grp"),
            P("col", "grp"),
            P("col", "grp"),
            P("grp", "col"),
            P("grp", "col"),
        ),
        check_vma=False,
    )
```
